256 devices in a mesh: row: 16 (over z, core), col: 16 (over x, y).
Axes of the slice: x: 4, y: 4, z: 8, core: 2. Of those that a mesh axis runs over, the one named last changes fastest.
Arguments:
- right_side: float32 [1, 16, 4, 1024], P(None, 'row'), may hold values from -6 to 6
- inverse_t: bfloat16 [1, 16, 1024, 1024], P(None, 'row', 'col'), as said below
- u_factor: bfloat16 [1, 16, 1, 16, 128, 1024], P(None, 'row', None, 'col'), may hold values from -0.25 to 0.25
- v_factor: bfloat16 [1, 16, 1, 16, 128, 1024], P(None, 'row', None, 'col'), may hold values from -0.1875 to 0.1875
- ranks: int32 [1, 16, 1, 16], P(None, 'row', None, 'col'), may hold values from 4 to 128, as said below
Outputs:
- whitened: float32 [1, 16, 4, 1024], P(None, 'row')
- loglik: float32 [1, 16, 4], P(None, 'row')
The draws below stay inside these ranges and needn't reach their ends.
Inputs may be any that keep to these rules, and one draw needn't show every extreme that they name: Tile (i, j) with j < i uses the first ranks of its factor rows. `inverse_t`: upper triangular with a positive diagonal.
All inputs are finite; a program needn't handle non-finite values.
Results may differ from the reference program's by a relative error of at most 0.0085.
Values sent between devices are 32-bit elements; how exact they have to be, the bound alone decides.
No kernel may reach another device: no remote copies, remote signals or barrier semaphores. Data moves between devices by JAX's collectives and lax.ppermute only.
A program may use at most 64 MiB of HBM per device.

```python
import math
import jax
import jax.numpy as jnp

NB = 1024
RMAX = 128
NRHS = 4
CYC = 1
SLAB = 16
N_ROW = 16
N_COL = 16


def draw_inverse_t(key, part):
    key_diag, key_off = jax.random.split(jax.random.fold_in(key, 11))
    shape = (CYC, N_ROW, NB, NB)
    diagonal = jnp.exp(jax.random.uniform(key_diag, (CYC, N_ROW, NB), jnp.float32, math.log(0.3), math.log(1.2)))
    spread = jax.random.normal(key_off, shape, jnp.float32)
    upper = jnp.triu(spread * (0.3 / math.sqrt(NB)), 1)
    eye = jnp.eye(NB, dtype=jnp.float32)
    matrix = upper + eye[None, None, :, :] * diagonal[:, :, :, None]
    return matrix.astype(jnp.bfloat16)


def draw_ranks(key, part):
    slab = CYC * N_ROW
    tile_cols = slab // N_COL
    shape = (CYC, N_ROW, tile_cols, N_COL)
    row_ids = jnp.arange(CYC, dtype=jnp.int32)[:, None, None, None] * N_ROW + jnp.arange(N_ROW, dtype=jnp.int32)[None, :, None, None]
    col_ids = jnp.arange(tile_cols, dtype=jnp.int32)[None, None, :, None] * N_COL + jnp.arange(N_COL, dtype=jnp.int32)[None, None, None, :]
    distance = jnp.maximum(row_ids - col_ids, 1)
    lowest = max(RMAX // 32, 1)
    highest = jnp.maximum(RMAX // distance, lowest)
    raw = jax.random.randint(jax.random.fold_in(key, 23), shape, 0, 1 << 20)
    values = lowest + raw % (highest - lowest + 1)
    forced = (row_ids == 1) & (col_ids == 0)
    values = jnp.where(forced, RMAX, values)
    return values.astype(jnp.int32)


def levels(rng, extent, shards, least, top_value):
    def one(position, parts):
        heights = jax.random.uniform(jax.random.fold_in(jax.random.fold_in(rng, 6), position), (parts,), jnp.float32, least / len(shards), top_value / len(shards))
        return jnp.repeat(jnp.exp(heights), extent[position] // parts).reshape((-1,) + (1,) * (len(extent) - position - 1))

    level = one(*shards[0])
    for cut in shards[1:]:
        level = level * one(*cut)
    return level


def scatter_about(own_key, dims, scale, bound, cuts=(), kind=jnp.bfloat16):
    loudness = levels(own_key, dims, cuts, -0.22, 0.18) if cuts else 1.0
    drawn = jax.random.normal(own_key, dims, jnp.float32) * scale * loudness
    return jnp.minimum(jnp.maximum(drawn, -bound), bound).astype(kind)


def setup_inputs(seed: int = 0) -> dict:
    key_of = jax.random.split(jax.random.key(seed), 6)
    return {
        "right_side": scatter_about(key_of[0], (CYC, N_ROW, NRHS, NB), 1.0, 6.0, ((1, 16),), jnp.float32),
        "inverse_t": draw_inverse_t(jax.random.fold_in(key_of[5], 71), 0),
        "u_factor": scatter_about(key_of[2], (CYC, N_ROW, SLAB // N_COL, N_COL, RMAX, NB), (4 * RMAX) ** -0.5, 0.25, ((1, 16), (3, 16))),
        "v_factor": scatter_about(key_of[3], (CYC, N_ROW, SLAB // N_COL, N_COL, RMAX, NB), NB ** -0.5, 0.1875, ((1, 16), (3, 16))),
        "ranks": draw_ranks(jax.random.fold_in(key_of[5], 71), 0),
    }


def reference(right_side, inverse_t, u_factor, v_factor, ranks):
    slab = CYC * N_ROW
    sources = right_side.reshape(slab, NRHS, NB)
    inverse = inverse_t.reshape(slab, NB, NB)
    u_tiles = u_factor.reshape(slab, slab, RMAX, NB)
    v_tiles = v_factor.reshape(slab, slab, RMAX, NB)
    limits = ranks.reshape(slab, slab)
    rank_index = jnp.arange(RMAX, dtype=jnp.int32)
    tile_index = jnp.arange(slab, dtype=jnp.int32)
    solved = jnp.zeros((slab, NRHS, NB), jnp.float32)
    for row in range(slab):
        rounded = solved.astype(jnp.bfloat16).astype(jnp.float32)
        inner = jnp.einsum('jrn,jkn->jrk', v_tiles[row].astype(jnp.float32), rounded)
        keep = (rank_index[None, :] < limits[row][:, None]) & (tile_index < row)[:, None]
        inner = jnp.where(keep[:, :, None], inner, 0.0).astype(jnp.bfloat16)
        partial_value = jnp.einsum('jrk,jrn->kn', inner.astype(jnp.float32), u_tiles[row].astype(jnp.float32))
        reduced = (sources[row] - partial_value).astype(jnp.bfloat16)
        result = jnp.dot(reduced, inverse[row], preferred_element_type=jnp.float32)
        solved = solved.at[row].set(result)
    diagonal = jnp.diagonal(inverse, axis1=1, axis2=2).astype(jnp.float32)
    logdiag = jnp.mean(jnp.log(diagonal), axis=1)
    quadratic = jnp.mean(solved * solved, axis=2)
    loglik = -0.5 * quadratic + logdiag[:, None] - 0.5 * math.log(2.0 * math.pi)
    return solved.reshape(CYC, N_ROW, NRHS, NB), loglik.reshape(CYC, N_ROW, NRHS)
```

```python
import math

import jax
import jax.numpy as jnp
from jax import lax
from jax.sharding import PartitionSpec as P

ROW = "row"
COL = "col"
BOTH = (ROW, COL)
SIDE = 4
CHAIN_PERIOD = 8
SPREAD_PERIOD = 7
ARRIVAL = {2: 0, 3: 1, 4: 1, 5: 2, 6: 2, 7: 2, 8: 3, 9: 3, 10: 3, 11: 3, 12: 4, 13: 4, 14: 4, 15: 4}
SENDER = {2: 1, 3: 1, 4: 2, 5: 1, 6: 2, 7: 4, 8: 1, 9: 2, 10: 4, 11: 6, 12: 1, 13: 2, 14: 4, 15: 6}


def solver(i):
    return (i, max(i - 1, 0))


def union(rounds, period):
    patterns = []
    for first in range(min(period, len(rounds))):
        pairs = sorted({pair for moves in rounds[first::period] for pair in moves})
        assert len({s for s, _ in pairs}) == len(pairs) == len({d for _, d in pairs})
        patterns.append(pairs)
    return [patterns[r % period] for r in range(len(rounds))]


def plan(n):
    chain, spread, gather = [], [], []
    for r in range(n - 1):
        chain.append([(solver(r), solver(r + 1))])
        spread_moves, gather_moves = [], []
        for i in range(n):
            for j in range(i - 1):
                d = i - j
                if j + ARRIVAL[d] == r:
                    source = solver(j) if SENDER[d] == 1 else (j + SENDER[d], j)
                    spread_moves.append((source, (i, j)))
                if i - 1 - (d - 2) // 2 == r:
                    (spread_moves if d % 2 else gather_moves).append(((i, j), solver(i)))
        spread.append(spread_moves)
        gather.append(gather_moves)
    return union(chain, CHAIN_PERIOD), union(spread, SPREAD_PERIOD), union(gather, SPREAD_PERIOD)


def local(right_side, inverse_t, u_factor, v_factor, ranks):
    n = lax.axis_size(ROW)
    n_col = lax.axis_size(COL)
    nrhs, width = right_side.shape[2:]
    piece = width // n_col
    quarter = width // SIDE
    rank_max = u_factor.shape[4]
    row = lax.axis_index(ROW)
    col = lax.axis_index(COL)
    source = right_side.reshape(nrhs, width)
    u_tile = u_factor.reshape(rank_max, width)
    v_tile = v_factor.reshape(rank_max, width)
    limit = ranks.reshape(1, 1)

    def move(array, pairs):
        numbered = [(s[0] * n_col + s[1], d[0] * n_col + d[1]) for s, d in pairs]
        return lax.ppermute(array, BOTH, numbered)

    def home(r):
        return divmod(solver(r)[1], SIDE)

    rows = inverse_t.reshape(piece, width).astype(jnp.float32)
    slabs = []
    for k in range(SIDE):
        pairs = []
        for r in range(n):
            for x in range(SIDE):
                if home(r)[1] != k:
                    pairs.append(((r, x * SIDE + k), (r, x * SIDE + home(r)[1])))
        slabs.append(move(rows, pairs) + jnp.where(col % SIDE == k, rows, 0.0))
    block = jnp.concatenate(slabs, axis=0)
    quarters = []
    for k in range(SIDE):
        pairs = []
        for r in range(n):
            x, y = home(r)
            if x != k:
                pairs.append(((r, k * SIDE + y), (r, x * SIDE + y)))
        part = block[:, k * quarter :]
        got = (move(part, pairs) + jnp.where(col // SIDE == k, part, 0.0)).astype(jnp.bfloat16)
        quarters.append(jnp.pad(got, ((0, 0), (k * quarter, 0))))
    inverse = lax.optimization_barrier(jnp.concatenate(quarters, axis=0))

    gap = row - col
    solves = (gap == 1) | ((row == 0) & (col == 0))
    keep = jnp.arange(rank_max, dtype=jnp.int32)[:, None] < limit

    def contribution(known):
        inner = jnp.einsum("rn,kn->rk", v_tile, known.astype(jnp.bfloat16), preferred_element_type=jnp.float32)
        inner = jnp.where(keep, inner, 0.0).astype(jnp.bfloat16)
        return jnp.einsum("rk,rn->kn", inner, u_tile, preferred_element_type=jnp.float32)

    def solve(known, pending):
        own = contribution(known)
        reduced = (source - pending - own).astype(jnp.bfloat16)
        return own, jnp.dot(reduced, inverse, preferred_element_type=jnp.float32)

    arrival = jnp.zeros((), jnp.int32)
    for d, when in ARRIVAL.items():
        arrival = jnp.where(gap == d, when, arrival)
    chain, spread, gather = plan(n)
    known = jnp.zeros((nrhs, width), jnp.float32)
    pending = jnp.zeros((nrhs, width), jnp.float32)
    own, result = solve(known, pending)
    for r in range(n - 1):
        behind = row - 1 - r
        first = move(result, chain[r])
        third = move(own, gather[r])
        second = move(jnp.where(solves, result, jnp.where(gap % 2 == 1, own, known)), spread[r])
        takes = (gap == 1) & (col == r)
        hears = (gap >= 2) & (col + arrival == r)
        adds = (gap == 1) & (behind >= 0)
        adds_odd = adds & (3 + 2 * behind <= row)
        adds_even = adds & (2 + 2 * behind <= row)
        known = known + jnp.where(takes, first, 0.0) + jnp.where(hears, second, 0.0)
        pending = pending + jnp.where(adds_odd, second, 0.0) + jnp.where(adds_even, third, 0.0)
        own, result = solve(known, pending)

    square = lax.dynamic_slice_in_dim(rows, col * piece, piece, 1)
    log_sum = jnp.sum(jnp.log(jnp.diagonal(square)))
    payload = jnp.concatenate([result, jnp.broadcast_to(log_sum, (nrhs, 128))], axis=1)
    payload = jnp.broadcast_to(payload[None], (n_col, *payload.shape))
    arrived = lax.all_to_all(payload, COL, 0, 0, tiled=True)
    solved = lax.dynamic_index_in_dim(arrived, jnp.maximum(row - 1, 0), 0, False)[:, :width]
    logdiag = jnp.sum(arrived[:, 0, width]) / width
    quadratic = jnp.mean(solved * solved, axis=1)
    loglik = -0.5 * quadratic + logdiag - 0.5 * math.log(2.0 * math.pi)
    return solved.reshape(1, 1, nrhs, width), loglik.reshape(1, 1, nrhs)


def solution(mesh):
    return jax.shard_map(
        local,
        mesh=mesh,
        in_specs=(
            P(None, ROW, None, None),
            P(None, ROW, COL, None),
            P(None, ROW, None, COL, None, None),
            P(None, ROW, None, COL, None, None),
            P(None, ROW, None, COL),
        ),
        out_specs=(P(None, ROW, None, None), P(None, ROW, None)),
        check_vma=False,
    )
```

```python
import math

import jax
import jax.numpy as jnp
from jax import lax
from jax.experimental import pallas as pl
from jax.experimental.pallas import tpu as pltpu
from jax.sharding import PartitionSpec as P


ROW = "row"
COL = "col"
BOTH = (ROW, COL)
SIDE = 4
BAND = 2
PERIOD = 7
SPREAD_PERIOD = 5
ARRIVAL = {3: 0, 4: 1, 5: 1, 6: 2, 7: 2, 8: 2, 9: 2, 10: 3, 11: 3, 12: 3, 13: 3, 14: 3, 15: 3}
SENDER = {3: 1, 4: 1, 5: 3, 6: 1, 7: 3, 8: 4, 9: 5, 10: 1, 11: 3, 12: 4, 13: 5, 14: 6, 15: 7}


def solver(i):
    return (i, i - 1 if i else 1)


def union(rounds, period):
    patterns = []
    for first in range(min(period, len(rounds))):
        pairs = sorted({pair for moves in rounds[first::period] for pair in moves})
        assert len({s for s, _ in pairs}) == len(pairs) == len({d for _, d in pairs})
        patterns.append(pairs)
    return [patterns[r % period] for r in range(len(rounds))]


def plan(n):
    chain, spread, odd, even = [], [], [], []
    for r in range(n - 1):
        chain.append([(solver(r), solver(r + 1))])
        spread.append([])
        odd.append([])
        even.append([])
        for i in range(n):
            for j in range(i - BAND):
                d = i - j
                if j + ARRIVAL[d] == r:
                    spread[r].append((solver(j) if SENDER[d] == 1 else (j + SENDER[d], j), (i, j)))
                if i - 2 - (d - 3) // 2 == r:
                    (odd if d % 2 else even)[r].append(((i, j), solver(i)))
    return union(chain, PERIOD), union(spread, SPREAD_PERIOD), union(odd, PERIOD), union(even, PERIOD)


def assemble(place, block, parts):
    quarter, width = block.shape

    def body(place_ref, block_ref, *refs):
        out = refs[-1]
        for k in range(SIDE):
            start = k * quarter
            got = refs[k][...] + jnp.where(place_ref[0] == k, block_ref[:, start:], 0.0)
            if start:
                out[start : start + quarter, :start] = jnp.zeros((quarter, start), jnp.bfloat16)
            out[start : start + quarter, start:] = got.astype(jnp.bfloat16)

    vmem = pl.BlockSpec(memory_space=pltpu.VMEM)
    return pl.pallas_call(
        body,
        in_specs=[pl.BlockSpec(memory_space=pltpu.SMEM)] + [vmem] * (1 + SIDE),
        out_specs=vmem,
        out_shape=jax.ShapeDtypeStruct((width, width), jnp.bfloat16),
        compiler_params=pltpu.CompilerParams(vmem_limit_bytes=16 * 2**20),
        name="assemble",
    )(place, block, *parts)


def step(r, where, came, heard, odds, evens, state, source, v_band, u_band, inverse):
    held = max(1, min(BAND, r + 1))
    nrhs, width = source.shape
    block = 256

    def body(round_ref, where_ref, came_ref, heard_ref, odds_ref, evens_ref, state_ref, source_ref, *refs):
        v_refs, u_refs = refs[:held], refs[held : 2 * held]
        inverse_ref, bundle_ref, spread_ref, own_ref, after_ref = refs[2 * held :]
        now = round_ref[0]
        row, col, arrival = where_ref[0], where_ref[1], where_ref[2]
        gap = row - col
        solves = (gap == 1) | ((row == 0) & (col == 1))
        takes = (gap == 1) & (col == now)
        hears = (gap > BAND) & (col + arrival == now)
        behind = row - 1 - now
        adds = (gap == 1) & (behind >= 0) & (now >= 1)
        adds_odd = adds & (3 + 2 * behind <= row)
        adds_even = adds & (4 + 2 * behind <= row)
        ys = []
        for d in range(BAND):
            y = state_ref[d] + jnp.where(takes, came_ref[d], 0.0)
            if d == 0:
                y = y + jnp.where(hears, heard_ref[...], 0.0)
            ys.append(y)
            after_ref[d] = y
        pending = state_ref[BAND] + jnp.where(adds_odd, odds_ref[...], 0.0) + jnp.where(adds_even, evens_ref[...], 0.0)
        after_ref[BAND] = pending
        total = source_ref[...] - pending
        inners = [
            lax.dot_general(ys[d].astype(jnp.bfloat16), v_refs[d][...], (((1,), (1,)), ((), ())), preferred_element_type=jnp.float32)
            for d in range(held)
        ]
        for d in range(held):
            part = jnp.dot(inners[d].astype(jnp.bfloat16), u_refs[d][...], preferred_element_type=jnp.float32)
            if d == 0:
                own_ref[...] = part
            total = total - part
        reduced = total.astype(jnp.bfloat16)
        columns = []
        for n in range(0, width, block):
            columns.append(
                jnp.dot(reduced[:, : n + block], inverse_ref[: n + block, n : n + block], preferred_element_type=jnp.float32)
            )
        result = jnp.concatenate(columns, axis=1)
        bundle_ref[0] = result
        for d in range(BAND - 1):
            bundle_ref[d + 1] = ys[d]
        spread_ref[...] = jnp.where(solves, result, ys[0])

    vmem = pl.BlockSpec(memory_space=pltpu.VMEM)
    smem = pl.BlockSpec(memory_space=pltpu.SMEM)
    small = jax.ShapeDtypeStruct((nrhs, width), jnp.float32)
    return pl.pallas_call(
        body,
        in_specs=[smem, smem] + [vmem] * (6 + 2 * held + 1),
        out_specs=[vmem] * 4,
        out_shape=[
            jax.ShapeDtypeStruct((BAND, nrhs, width), jnp.float32),
            small,
            small,
            jax.ShapeDtypeStruct((BAND + 1, nrhs, width), jnp.float32),
        ],
        compiler_params=pltpu.CompilerParams(vmem_limit_bytes=8 * 2**20),
        name="step",
    )(jnp.full((1,), r, jnp.int32), where, came, heard, odds, evens, state, source, *v_band[:held], *u_band[:held], inverse)


def local(right_side, inverse_t, u_factor, v_factor, ranks):
    n = lax.axis_size(ROW)
    n_col = lax.axis_size(COL)
    nrhs, width = right_side.shape[2:]
    piece = width // n_col
    rank_max = u_factor.shape[4]
    row = lax.axis_index(ROW)
    col = lax.axis_index(COL)
    gap = row - col
    source = right_side.reshape(nrhs, width)
    u_tile = u_factor.reshape(rank_max, width)
    v_tile = v_factor.reshape(rank_max, width)
    keep = jnp.arange(rank_max, dtype=jnp.int32)[:, None] < ranks.reshape(1, 1)
    u_tile = jnp.where(keep, u_tile, jnp.zeros_like(u_tile))

    def move(array, pairs):
        numbered = [(s[0] * n_col + s[1], d[0] * n_col + d[1]) for s, d in pairs]
        return lax.ppermute(array, BOTH, numbered)

    rows = inverse_t.reshape(piece, width).astype(jnp.float32)
    quarter = width // SIDE
    slabs = []
    for k in range(SIDE):
        pairs = [
            ((r, x * SIDE + k), (r, x * SIDE + solver(r)[1] % SIDE))
            for r in range(n)
            for x in range(SIDE)
            if solver(r)[1] % SIDE != k
        ]
        slabs.append(move(rows, pairs) + jnp.where(col % SIDE == k, rows, 0.0))
    square = lax.dynamic_slice_in_dim(rows, col * piece, piece, 1)
    log_sum = jnp.sum(jnp.log(jnp.diagonal(square)))
    both = jnp.concatenate([v_tile, u_tile], axis=0).astype(jnp.float32)
    block, both, log_sum = lax.optimization_barrier((jnp.concatenate(slabs, axis=0), both, log_sum))
    parts = []
    for k in range(SIDE):
        pairs = [
            ((r, k * SIDE + solver(r)[1] % SIDE), solver(r)) for r in range(n) if solver(r)[1] // SIDE != k
        ]
        parts.append(move(block[:, k * quarter :], pairs))
    place = jnp.stack([col // SIDE]).astype(jnp.int32)

    second = move(both, [((i, i - 2), solver(i)) for i in range(2, n)])
    inverse = assemble(place, block, parts)
    second = (second + jnp.where(gap == 1, 0.0, both)).astype(jnp.bfloat16)
    v_band = [v_tile, second[:rank_max]]
    u_band = [u_tile, second[rank_max:]]

    arrival = jnp.full((), 99, jnp.int32)
    for d, when in ARRIVAL.items():
        arrival = jnp.where(gap == d, when, arrival)
    chain, spread, odd, even = plan(n)
    where = jnp.stack([row, col, arrival]).astype(jnp.int32)
    nothing = jnp.zeros((nrhs, width), jnp.float32)
    state = jnp.zeros((BAND + 1, nrhs, width), jnp.float32)
    no_bundle = jnp.zeros((BAND, nrhs, width), jnp.float32)
    bundle, spread_out, own, state = step(
        -1, where, no_bundle, nothing, nothing, nothing, state, source, v_band, u_band, inverse
    )
    odds = evens = nothing
    for r in range(n - 1):
        came = move(bundle, chain[r])
        heard = more_odds = more_evens = nothing
        if spread[r]:
            heard = move(spread_out, spread[r])
        if 1 <= r < n - 2:
            more_odds = move(own, odd[r])
        if 2 <= r < n - 2:
            more_evens = move(own, even[r])
        bundle, spread_out, own, state = step(
            r, where, came, heard, odds, evens, state, source, v_band, u_band, inverse
        )
        odds, evens = more_odds, more_evens
    result = bundle[0]

    payload = jnp.concatenate([result, jnp.broadcast_to(log_sum, (nrhs, 128))], axis=1)
    payload = jnp.broadcast_to(payload[None], (n_col, *payload.shape))
    arrived = lax.all_to_all(payload, COL, 0, 0, tiled=True)
    solved = lax.dynamic_index_in_dim(arrived, jnp.where(row == 0, 1, row - 1), 0, False)[:, :width]
    logdiag = jnp.sum(arrived[:, 0, width]) / width
    quadratic = jnp.mean(solved * solved, axis=1)
    loglik = -0.5 * quadratic + logdiag - 0.5 * math.log(2.0 * math.pi)
    return solved.reshape(1, 1, nrhs, width), loglik.reshape(1, 1, nrhs)


def solution(mesh):
    return jax.shard_map(
        local,
        mesh=mesh,
        in_specs=(
            P(None, ROW, None, None),
            P(None, ROW, COL, None),
            P(None, ROW, None, COL, None, None),
            P(None, ROW, None, COL, None, None),
            P(None, ROW, None, COL),
        ),
        out_specs=(P(None, ROW, None, None), P(None, ROW, None)),
        check_vma=False,
    )
```

```python
import math

import jax
import jax.numpy as jnp
from jax import lax
from jax.experimental import pallas as pl
from jax.experimental.pallas import tpu as pltpu
from jax.sharding import Mesh
from jax.sharding import PartitionSpec as P


ROW = "row"
COL = ("col_x", "col_y")
BOTH = (ROW, *COL)
SIDE = 4
BAND = 2
CHAIN_PERIOD = 5
SPREAD_PERIOD = 7
FAR_PERIOD = 7
ARRIVAL = {3: 0, 4: 1, 5: 1, 6: 2, 7: 2, 8: 2, 9: 3, 10: 3, 11: 3, 12: 3, 13: 3, 14: 3, 15: 4}
SENDER = {3: 1, 4: 1, 5: 3, 6: 3, 7: 4, 8: 5, 9: 3, 10: 4, 11: 5, 12: 6, 13: 7, 14: 8, 15: 3}


def solver(i):
    return (i, i - 1 if i else 1)


def union(rounds, period):
    patterns = []
    for first in range(min(period, len(rounds))):
        pairs = sorted({pair for moves in rounds[first::period] for pair in moves})
        assert len({s for s, _ in pairs}) == len(pairs) == len({d for _, d in pairs})
        patterns.append(pairs)
    return [patterns[r % period] for r in range(len(rounds))]


def plan(n):
    chain, spread, odd, even = [], [], [], []
    for r in range(n - 1):
        chain.append([(solver(r), solver(r + 1))])
        spread.append([])
        odd.append([])
        even.append([])
        for i in range(n):
            for j in range(i - BAND):
                d = i - j
                if j + ARRIVAL[d] == r:
                    spread[r].append((solver(j) if SENDER[d] == 1 else (j + SENDER[d], j), (i, j)))
                if i - 2 - (d - 3) // 2 == r:
                    (odd if d % 2 else even)[r].append(((i, j), solver(i)))
    return (
        union(chain, CHAIN_PERIOD),
        union(spread, SPREAD_PERIOD),
        union(odd, FAR_PERIOD),
        union(even, FAR_PERIOD),
    )


def assemble(place, block, parts):
    quarter, width = block.shape

    def body(place_ref, block_ref, *refs):
        out = refs[-1]
        for k in range(SIDE):
            start = k * quarter
            got = refs[k][...] + jnp.where(place_ref[0] == k, block_ref[:, start:], 0.0)
            if start:
                out[start : start + quarter, :start] = jnp.zeros((quarter, start), jnp.bfloat16)
            out[start : start + quarter, start:] = got.astype(jnp.bfloat16)

    vmem = pl.BlockSpec(memory_space=pltpu.VMEM)
    return pl.pallas_call(
        body,
        in_specs=[pl.BlockSpec(memory_space=pltpu.SMEM)] + [vmem] * (1 + SIDE),
        out_specs=vmem,
        out_shape=jax.ShapeDtypeStruct((width, width), jnp.bfloat16),
        compiler_params=pltpu.CompilerParams(vmem_limit_bytes=16 * 2**20),
        name="assemble",
    )(place, block, *parts)


def step(now, came, heard, odds, evens, value, own, pending, source, v_band, u_band, inverse):
    held = 1 if now < 1 else BAND
    nrhs, width = source.shape
    block = 256

    def body(came_ref, heard_ref, odds_ref, evens_ref, value_ref, own_ref, pending_ref, source_ref, *refs):
        v_refs, u_refs = refs[:held], refs[held : 2 * held]
        inverse_ref, bundle_out, value_out, own_out, pending_out = refs[2 * held :]
        row = lax.axis_index(ROW)
        col = lax.axis_index(COL[0]) * SIDE + lax.axis_index(COL[1])
        gap = row - col
        if now < 0:
            turn = (row == 0) & (col == 1)
        else:
            turn = (row == now + 1) & (gap == 1)
        hears = row < 0
        for when in sorted(set(ARRIVAL.values())):
            gaps = [d for d in ARRIVAL if ARRIVAL[d] == when]
            hears = hears | ((gap >= min(gaps)) & (gap <= max(gaps)) & (col == now - when))
        behind = row - 1 - now
        adds = (gap == 1) & (behind >= 0)
        left = pending_ref[...]
        if now >= 2:
            left = left + jnp.where(adds & (3 + 2 * behind <= row), odds_ref[...], 0.0)
        if now >= 3:
            left = left + jnp.where(adds & (4 + 2 * behind <= row), evens_ref[...], 0.0)
        pending_out[...] = left

        def share(known, d):
            inner = lax.dot_general(
                known.astype(jnp.bfloat16), v_refs[d][...], (((1,), (1,)), ((), ())), preferred_element_type=jnp.float32
            )
            return jnp.dot(inner.astype(jnp.bfloat16), u_refs[d][...], preferred_element_type=jnp.float32)

        @pl.when(jnp.logical_not(turn | hears))
        def _():
            value_out[...] = value_ref[...]
            own_out[...] = own_ref[...]

        @pl.when(hears)
        def _():
            value_out[...] = heard_ref[...]
            own_out[...] = share(heard_ref[...], 0)

        @pl.when(turn)
        def _():
            total = source_ref[...] - left
            if now >= 0:
                for d in range(held):
                    total = total - share(came_ref[d], d)
                bundle_out[1] = came_ref[0]
            else:
                bundle_out[1] = jnp.zeros((nrhs, width), jnp.float32)
            reduced = total.astype(jnp.bfloat16)
            columns = []
            for n in range(0, width, block):
                columns.append(
                    jnp.dot(
                        reduced[:, : n + block],
                        inverse_ref[: n + block, n : n + block],
                        preferred_element_type=jnp.float32,
                    )
                )
            result = jnp.concatenate(columns, axis=1)
            bundle_out[0] = result
            value_out[...] = result
            own_out[...] = own_ref[...]

    vmem = pl.BlockSpec(memory_space=pltpu.VMEM)
    small = jax.ShapeDtypeStruct((nrhs, width), jnp.float32)
    return pl.pallas_call(
        body,
        in_specs=[vmem] * (8 + 2 * held + 1),
        out_specs=[vmem] * 4,
        out_shape=[jax.ShapeDtypeStruct((BAND, nrhs, width), jnp.float32), small, small, small],
        compiler_params=pltpu.CompilerParams(vmem_limit_bytes=8 * 2**20),
        name="step",
    )(came, heard, odds, evens, value, own, pending, source, *v_band[:held], *u_band[:held], inverse)


def local(right_side, inverse_t, u_factor, v_factor, ranks):
    n = lax.axis_size(ROW)
    n_col = lax.axis_size(COL)
    nrhs, width = right_side.shape[2:]
    piece = width // n_col
    rank_max = u_factor.shape[4]
    row = lax.axis_index(ROW)
    col = lax.axis_index(COL)
    gap = row - col
    source = right_side.reshape(nrhs, width)
    u_tile = u_factor.reshape(rank_max, width)
    v_tile = v_factor.reshape(rank_max, width)
    keep = jnp.arange(rank_max, dtype=jnp.int32)[:, None] < ranks.reshape(1, 1)
    u_tile = jnp.where(keep, u_tile, jnp.zeros_like(u_tile))

    def move(array, pairs):
        numbered = [(s[0] * n_col + s[1], d[0] * n_col + d[1]) for s, d in pairs]
        return lax.ppermute(array, BOTH, numbered)

    rows = inverse_t.reshape(piece, width).astype(jnp.float32)
    quarter = width // SIDE
    slabs = []
    for k in range(SIDE):
        pairs = [
            ((r, x * SIDE + k), (r, x * SIDE + solver(r)[1] % SIDE))
            for r in range(n)
            for x in range(SIDE)
            if solver(r)[1] % SIDE != k
        ]
        slabs.append(move(rows, pairs) + jnp.where(col % SIDE == k, rows, 0.0))
    block = jnp.concatenate(slabs, axis=0)
    square = lax.dynamic_slice_in_dim(rows, col * piece, piece, 1)
    log_sum = jnp.sum(jnp.log(jnp.diagonal(square)))
    both = jnp.concatenate([v_tile, u_tile], axis=0).astype(jnp.float32)
    block, both, log_sum = lax.optimization_barrier((block, both, log_sum))
    parts = []
    for k in range(SIDE):
        pairs = [
            ((r, k * SIDE + solver(r)[1] % SIDE), solver(r)) for r in range(n) if solver(r)[1] // SIDE != k
        ]
        parts.append(move(block[:, k * quarter :], pairs))
    place = jnp.stack([col // SIDE]).astype(jnp.int32)

    second = move(both, [((i, i - 2), solver(i)) for i in range(2, n)])
    inverse = assemble(place, block, parts)
    second = (second + jnp.where(gap == 1, 0.0, both)).astype(jnp.bfloat16)
    v_band = [v_tile, second[:rank_max]]
    u_band = [u_tile, second[rank_max:]]

    chain, spread, odd, even = plan(n)
    nothing = jnp.zeros((nrhs, width), jnp.float32)
    no_bundle = jnp.zeros((BAND, nrhs, width), jnp.float32)
    bundle, value, own, pending = step(
        -1, no_bundle, nothing, nothing, nothing, nothing, nothing, nothing, source, v_band, u_band, inverse
    )
    odds = evens = nothing
    for r in range(n - 1):
        came = move(bundle, chain[r])
        heard = more_odds = more_evens = nothing
        if spread[r]:
            heard = move(value, spread[r])
        if 1 <= r < n - 2:
            more_odds = move(own, odd[r])
        if 2 <= r < n - 2:
            more_evens = move(own, even[r])
        bundle, value, own, pending = step(
            r, came, heard, odds, evens, value, own, pending, source, v_band, u_band, inverse
        )
        odds, evens = more_odds, more_evens
    result = value

    payload = jnp.concatenate([result, jnp.broadcast_to(log_sum, (nrhs, 128))], axis=1)
    payload = jnp.broadcast_to(payload[None], (n_col, *payload.shape))
    arrived = lax.all_to_all(payload, COL, 0, 0, tiled=True)
    solved = lax.dynamic_index_in_dim(arrived, jnp.where(row == 0, 1, row - 1), 0, False)[:, :width]
    logdiag = jnp.sum(arrived[:, 0, width]) / width
    quadratic = jnp.mean(solved * solved, axis=1)
    loglik = -0.5 * quadratic + logdiag - 0.5 * math.log(2.0 * math.pi)
    return solved.reshape(1, 1, nrhs, width), loglik.reshape(1, 1, nrhs)


def solution(mesh):
    plane = Mesh(mesh.devices.reshape(-1, SIDE, SIDE), BOTH)
    return jax.shard_map(
        local,
        mesh=plane,
        in_specs=(
            P(None, ROW, None, None),
            P(None, ROW, COL, None),
            P(None, ROW, None, COL, None, None),
            P(None, ROW, None, COL, None, None),
            P(None, ROW, None, COL),
        ),
        out_specs=(P(None, ROW, None, None), P(None, ROW, None)),
        check_vma=False,
    )
```

```python
import math

import jax
import jax.numpy as jnp
from jax import lax
from jax.experimental import pallas as pl
from jax.experimental.pallas import tpu as pltpu
from jax.sharding import Mesh
from jax.sharding import PartitionSpec as P


ROW = "row"
COL = ("col_x", "col_y")
BOTH = (ROW, *COL)
SIDE = 4
BAND = 3
CHAIN_PERIOD = 13
FAR_PERIOD = 6
ARRIVAL = {4: 1, 5: 2, 6: 2, 7: 3, 8: 3, 9: 3, 10: 4, 11: 4, 12: 4, 13: 4, 14: 4, 15: 4}
SENDER = {4: 1, 5: 1, 6: 4, 7: 4, 8: 5, 9: 6, 10: 4, 11: 5, 12: 6, 13: 7, 14: 8, 15: 9}


def solver(i):
    return (i, i - 1 if i else 1)


def union(rounds, period):
    patterns = []
    for first in range(min(period, len(rounds))):
        pairs = sorted({pair for moves in rounds[first::period] for pair in moves})
        assert len({s for s, _ in pairs}) == len(pairs) == len({d for _, d in pairs})
        patterns.append(pairs)
    return [patterns[r % period] for r in range(len(rounds))]


def plan(n):
    chain, odd, even = [], [], []
    for r in range(n - 1):
        chain.append([(solver(r), solver(r + 1))])
        odd.append([])
        even.append([])
        for i in range(n):
            for j in range(i - BAND):
                d = i - j
                if j + ARRIVAL[d] == r:
                    chain[r].append((solver(j) if SENDER[d] == 1 else (j + SENDER[d], j), (i, j)))
                if i - 2 - (d - 4) // 2 == r:
                    (odd if d % 2 else even)[r].append(((i, j), solver(i)))
    return union(chain, CHAIN_PERIOD), union(odd, FAR_PERIOD), union(even, FAR_PERIOD)


def assemble(place, block, parts):
    quarter, width = block.shape

    def body(place_ref, block_ref, *refs):
        out = refs[-1]
        for k in range(SIDE):
            start = k * quarter
            got = refs[k][...] + jnp.where(place_ref[0] == k, block_ref[:, start:], 0.0)
            if start:
                out[start : start + quarter, :start] = jnp.zeros((quarter, start), jnp.bfloat16)
            out[start : start + quarter, start:] = got.astype(jnp.bfloat16)

    vmem = pl.BlockSpec(memory_space=pltpu.VMEM)
    return pl.pallas_call(
        body,
        in_specs=[pl.BlockSpec(memory_space=pltpu.SMEM)] + [vmem] * (1 + SIDE),
        out_specs=vmem,
        out_shape=jax.ShapeDtypeStruct((width, width), jnp.bfloat16),
        compiler_params=pltpu.CompilerParams(vmem_limit_bytes=16 * 2**20),
        name="assemble",
    )(place, block, *parts)


def step(now, came, odds, evens, send, own, pending, source, v_band, u_band, inverse):
    held = max(1, min(BAND, now + 1))
    nrhs, width = source.shape
    block = 256

    def body(came_ref, odds_ref, evens_ref, send_ref, own_ref, pending_ref, source_ref, *refs):
        v_refs, u_refs = refs[:held], refs[held : 2 * held]
        inverse_ref, send_out, own_out, pending_out = refs[2 * held :]
        row = lax.axis_index(ROW)
        col = lax.axis_index(COL[0]) * SIDE + lax.axis_index(COL[1])
        gap = row - col
        if now < 0:
            turn = (row == 0) & (col == 1)
        else:
            turn = (row == now + 1) & (gap == 1)
        hears = row < 0
        for when in sorted(set(ARRIVAL.values())):
            gaps = [d for d in ARRIVAL if ARRIVAL[d] == when]
            hears = hears | ((gap >= min(gaps)) & (gap <= max(gaps)) & (col == now - when))
        behind = row - 1 - now
        adds = (gap == 1) & (behind >= 0)
        left = pending_ref[...]
        if now >= 3:
            left = left + jnp.where(adds & (4 + 2 * behind <= row), evens_ref[...], 0.0)
        if now >= 4:
            left = left + jnp.where(adds & (5 + 2 * behind <= row), odds_ref[...], 0.0)
        pending_out[...] = left

        def share(known, d):
            inner = lax.dot_general(
                known.astype(jnp.bfloat16), v_refs[d][...], (((1,), (1,)), ((), ())), preferred_element_type=jnp.float32
            )
            return jnp.dot(inner.astype(jnp.bfloat16), u_refs[d][...], preferred_element_type=jnp.float32)

        @pl.when(jnp.logical_not(turn))
        def _():
            send_out[1] = jnp.zeros((nrhs, width), jnp.float32)
            send_out[2] = jnp.zeros((nrhs, width), jnp.float32)

        @pl.when(jnp.logical_not(turn | hears))
        def _():
            send_out[0] = send_ref[0]
            own_out[...] = own_ref[...]

        @pl.when(hears)
        def _():
            send_out[0] = came_ref[0]
            own_out[...] = share(came_ref[0], 0)

        @pl.when(turn)
        def _():
            total = source_ref[...] - left
            if now >= 0:
                for d in range(held):
                    total = total - share(came_ref[d], d)
            reduced = total.astype(jnp.bfloat16)
            columns = []
            for n in range(0, width, block):
                columns.append(
                    jnp.dot(
                        reduced[:, : n + block],
                        inverse_ref[: n + block, n : n + block],
                        preferred_element_type=jnp.float32,
                    )
                )
            send_out[0] = jnp.concatenate(columns, axis=1)
            for d in range(1, BAND):
                send_out[d] = came_ref[d - 1] if now >= 0 else jnp.zeros((nrhs, width), jnp.float32)
            own_out[...] = own_ref[...]

    vmem = pl.BlockSpec(memory_space=pltpu.VMEM)
    small = jax.ShapeDtypeStruct((nrhs, width), jnp.float32)
    return pl.pallas_call(
        body,
        in_specs=[vmem] * (7 + 2 * held + 1),
        out_specs=[vmem] * 3,
        out_shape=[jax.ShapeDtypeStruct((BAND, nrhs, width), jnp.float32), small, small],
        compiler_params=pltpu.CompilerParams(vmem_limit_bytes=8 * 2**20),
        name="step",
    )(came, odds, evens, send, own, pending, source, *v_band[:held], *u_band[:held], inverse)


def local(right_side, inverse_t, u_factor, v_factor, ranks):
    n = lax.axis_size(ROW)
    n_col = lax.axis_size(COL)
    nrhs, width = right_side.shape[2:]
    piece = width // n_col
    rank_max = u_factor.shape[4]
    row = lax.axis_index(ROW)
    col = lax.axis_index(COL)
    gap = row - col
    source = right_side.reshape(nrhs, width)
    u_tile = u_factor.reshape(rank_max, width)
    v_tile = v_factor.reshape(rank_max, width)
    keep = jnp.arange(rank_max, dtype=jnp.int32)[:, None] < ranks.reshape(1, 1)
    u_tile = jnp.where(keep, u_tile, jnp.zeros_like(u_tile))

    def move(array, pairs):
        numbered = [(s[0] * n_col + s[1], d[0] * n_col + d[1]) for s, d in pairs]
        return lax.ppermute(array, BOTH, numbered)

    rows = inverse_t.reshape(piece, width).astype(jnp.float32)
    quarter = width // SIDE
    slabs = []
    for k in range(SIDE):
        pairs = [
            ((r, x * SIDE + k), (r, x * SIDE + solver(r)[1] % SIDE))
            for r in range(n)
            for x in range(SIDE)
            if solver(r)[1] % SIDE != k
        ]
        slabs.append(move(rows, pairs) + jnp.where(col % SIDE == k, rows, 0.0))
    block = jnp.concatenate(slabs, axis=0)
    square = lax.dynamic_slice_in_dim(rows, col * piece, piece, 1)
    log_sum = jnp.sum(jnp.log(jnp.diagonal(square)))
    both = jnp.concatenate([v_tile, u_tile], axis=0).astype(jnp.float32)
    block, both, log_sum = lax.optimization_barrier((block, both, log_sum))
    parts = []
    for k in range(SIDE):
        pairs = [
            ((r, k * SIDE + solver(r)[1] % SIDE), solver(r)) for r in range(n) if solver(r)[1] // SIDE != k
        ]
        parts.append(move(block[:, k * quarter :], pairs))
    place = jnp.stack([col // SIDE]).astype(jnp.int32)

    v_band, u_band = [v_tile], [u_tile]
    moved = []
    for d in range(2, BAND + 1):
        moved.append(move(both, [((i, i - d), solver(i)) for i in range(d, n)]))
    inverse = assemble(place, block, parts)
    for tile in moved:
        tile = (tile + jnp.where(gap == 1, 0.0, both)).astype(jnp.bfloat16)
        v_band.append(tile[:rank_max])
        u_band.append(tile[rank_max:])

    chain, odd, even = plan(n)
    nothing = jnp.zeros((nrhs, width), jnp.float32)
    came = jnp.zeros((BAND, nrhs, width), jnp.float32)
    send, own, pending = step(-1, came, nothing, nothing, came, nothing, nothing, source, v_band, u_band, inverse)
    odds = evens = nothing
    for r in range(n - 1):
        came = move(send, chain[r])
        more_odds = more_evens = nothing
        if odd[r] and 3 <= r < n - 2:
            more_odds = move(own, odd[r])
        if even[r] and 2 <= r < n - 2:
            more_evens = move(own, even[r])
        send, own, pending = step(
            r, came, odds, evens, send, own, pending, source, v_band, u_band, inverse
        )
        odds, evens = more_odds, more_evens
    result = send[0]

    payload = jnp.concatenate([result, jnp.broadcast_to(log_sum, (nrhs, 128))], axis=1)
    payload = jnp.broadcast_to(payload[None], (n_col, *payload.shape))
    arrived = lax.all_to_all(payload, COL, 0, 0, tiled=True)
    solved = lax.dynamic_index_in_dim(arrived, jnp.where(row == 0, 1, row - 1), 0, False)[:, :width]
    logdiag = jnp.sum(arrived[:, 0, width]) / width
    quadratic = jnp.mean(solved * solved, axis=1)
    loglik = -0.5 * quadratic + logdiag - 0.5 * math.log(2.0 * math.pi)
    return solved.reshape(1, 1, nrhs, width), loglik.reshape(1, 1, nrhs)


def solution(mesh):
    plane = Mesh(mesh.devices.reshape(-1, SIDE, SIDE), BOTH)
    return jax.shard_map(
        local,
        mesh=plane,
        in_specs=(
            P(None, ROW, None, None),
            P(None, ROW, COL, None),
            P(None, ROW, None, COL, None, None),
            P(None, ROW, None, COL, None, None),
            P(None, ROW, None, COL),
        ),
        out_specs=(P(None, ROW, None, None), P(None, ROW, None)),
        check_vma=False,
    )
```

```python
import math

import jax
import jax.numpy as jnp
from jax import lax
from jax.experimental import pallas as pl
from jax.experimental.pallas import tpu as pltpu
from jax.sharding import Mesh
from jax.sharding import PartitionSpec as P


ROW = "row"
COL = ("col_x", "col_y")
BOTH = (ROW, *COL)
SIDE = 4
BAND = 3
CHAIN_PERIOD = 13
FAR_PERIOD = 6
ARRIVAL = {4: 1, 5: 2, 6: 2, 7: 3, 8: 3, 9: 3, 10: 4, 11: 4, 12: 4, 13: 4, 14: 4, 15: 4}
SENDER = {4: 1, 5: 1, 6: 4, 7: 4, 8: 5, 9: 6, 10: 4, 11: 5, 12: 6, 13: 7, 14: 8, 15: 9}


def solver(i):
    return (i, i - 1 if i else 1)


def union(rounds, period):
    patterns = []
    for first in range(min(period, len(rounds))):
        pairs = sorted({pair for moves in rounds[first::period] for pair in moves})
        assert len({s for s, _ in pairs}) == len(pairs) == len({d for _, d in pairs})
        patterns.append(pairs)
    return [patterns[r % period] for r in range(len(rounds))]


def plan(n):
    chain, odd, even = [], [], []
    for r in range(n - 1):
        chain.append([(solver(r), solver(r + 1))])
        odd.append([])
        even.append([])
        for i in range(n):
            for j in range(i - BAND):
                d = i - j
                if j + ARRIVAL[d] == r:
                    chain[r].append((solver(j) if SENDER[d] == 1 else (j + SENDER[d], j), (i, j)))
                if i - 2 - (d - 4) // 2 == r:
                    (odd if d % 2 else even)[r].append(((i, j), solver(i)))
    return union(chain, CHAIN_PERIOD), union(odd, FAR_PERIOD), union(even, FAR_PERIOD)


def assemble(place, block, parts):
    quarter, width = block.shape

    def body(place_ref, block_ref, *refs):
        out = refs[-1]
        for k in range(SIDE):
            start = k * quarter
            got = refs[k][...] + jnp.where(place_ref[0] == k, block_ref[:, start:], 0.0)
            if start:
                out[start : start + quarter, :start] = jnp.zeros((quarter, start), jnp.bfloat16)
            out[start : start + quarter, start:] = got.astype(jnp.bfloat16)

    vmem = pl.BlockSpec(memory_space=pltpu.VMEM)
    return pl.pallas_call(
        body,
        in_specs=[pl.BlockSpec(memory_space=pltpu.SMEM)] + [vmem] * (1 + SIDE),
        out_specs=vmem,
        out_shape=jax.ShapeDtypeStruct((width, width), jnp.bfloat16),
        compiler_params=pltpu.CompilerParams(vmem_limit_bytes=16 * 2**20),
        name="assemble",
    )(place, block, *parts)


VMEM = pl.BlockSpec(memory_space=pltpu.VMEM)
TO_ROWS = (((1,), (1,)), ((), ()))


def call(body, inputs, shapes, limit=8):
    return pl.pallas_call(
        body,
        in_specs=[VMEM] * len(inputs),
        out_specs=[VMEM] * len(shapes),
        out_shape=[jax.ShapeDtypeStruct(shape, dtype) for shape, dtype in shapes],
        compiler_params=pltpu.CompilerParams(vmem_limit_bytes=limit * 2**20),
    )(*inputs)


def here():
    row = lax.axis_index(ROW)
    col = lax.axis_index(COL[0]) * SIDE + lax.axis_index(COL[1])
    return row, col


def in_turn(now):
    row, col = here()
    if now < 0:
        return (row == 0) & (col == 1)
    return (row == now + 1) & (row - col == 1)


def through(lhs, inverse_ref, block=256):
    width = inverse_ref.shape[1]
    columns = [
        jnp.dot(lhs[:, : n + block], inverse_ref[: n + block, n : n + block], preferred_element_type=jnp.float32)
        for n in range(0, width, block)
    ]
    return jnp.concatenate(columns, axis=1)


def settle(factors, inverse):
    rank_max, width = factors.shape[0] // 2, factors.shape[1]

    def body(factors_ref, inverse_ref, v_out, u_out):
        v_out[...] = factors_ref[:rank_max].astype(jnp.bfloat16)
        u_out[...] = through(factors_ref[rank_max:].astype(jnp.bfloat16), inverse_ref).astype(jnp.bfloat16)

    shape = ((rank_max, width), jnp.bfloat16)
    return call(body, (factors, inverse), (shape, shape))


def prepare(now, odds, evens, pending, source, inverse):
    nrhs, width = source.shape

    def body(odds_ref, evens_ref, pending_ref, source_ref, inverse_ref, pending_out, base_out):
        row, col = here()
        behind = row - 1 - now
        adds = (row - col == 1) & (behind >= 0)
        left = pending_ref[...]
        if now >= 3:
            left = left + jnp.where(adds & (4 + 2 * behind <= row), evens_ref[...], 0.0)
        if now >= 4:
            left = left + jnp.where(adds & (5 + 2 * behind <= row), odds_ref[...], 0.0)
        pending_out[...] = left

        @pl.when(in_turn(now))
        def _():
            total = source_ref[...] - left
            high = total.astype(jnp.bfloat16)
            low = (total - high.astype(jnp.float32)).astype(jnp.bfloat16)
            base_out[...] = through(high, inverse_ref) + through(low, inverse_ref)

    small = ((nrhs, width), jnp.float32)
    return call(body, (odds, evens, pending, source, inverse), (small, small))


def step(now, came, send, own, base, v_tile, u_tile, v_band, u_band):
    held = max(0, min(BAND, now + 1))
    nrhs, width = base.shape

    def body(came_ref, send_ref, own_ref, base_ref, v_ref, u_ref, *refs):
        v_refs, u_refs = refs[:held], refs[held : 2 * held]
        send_out, own_out = refs[2 * held :]
        row, col = here()
        gap = row - col
        turn = in_turn(now)
        hears = row < 0
        for when in sorted(set(ARRIVAL.values())):
            gaps = [d for d in ARRIVAL if ARRIVAL[d] == when]
            hears = hears | ((gap >= min(gaps)) & (gap <= max(gaps)) & (col == now - when))

        def share(known, v, u):
            inner = lax.dot_general(known.astype(jnp.bfloat16), v[...], TO_ROWS, preferred_element_type=jnp.float32)
            return jnp.dot(inner.astype(jnp.bfloat16), u[...], preferred_element_type=jnp.float32)

        @pl.when(jnp.logical_not(turn))
        def _():
            for d in range(1, BAND):
                send_out[d] = jnp.zeros((nrhs, width), jnp.float32)

        @pl.when(jnp.logical_not(turn | hears))
        def _():
            send_out[0] = send_ref[0]
            own_out[...] = own_ref[...]

        @pl.when(hears)
        def _():
            send_out[0] = came_ref[0]
            own_out[...] = share(came_ref[0], v_ref, u_ref)

        @pl.when(turn)
        def _():
            total = base_ref[...]
            for d in range(held):
                total = total - share(came_ref[d], v_refs[d], u_refs[d])
            send_out[0] = total
            for d in range(1, BAND):
                send_out[d] = came_ref[d - 1]
            own_out[...] = own_ref[...]

    inputs = (came, send, own, base, v_tile, u_tile, *v_band[:held], *u_band[:held])
    return call(body, inputs, (((BAND, nrhs, width), jnp.float32), ((nrhs, width), jnp.float32)))


def spread_out(send, log_sum, n_col):
    nrhs, width = send.shape[1:]

    def body(send_ref, log_ref, out):
        for c in range(n_col):
            out[c, :, :width] = send_ref[0]
            out[c, :, width:] = log_ref[...]

    return call(body, (send, log_sum), (((n_col, nrhs, width + 128), jnp.float32),))[0]


def finish(arrived, width):
    n_col, nrhs = arrived.shape[:2]

    def body(arrived_ref, solved_out, loglik_out):
        row, _ = here()
        solved = arrived_ref[jnp.where(row == 0, 1, row - 1), :, :width]
        solved_out[...] = solved
        logs = arrived_ref[0, :, width:]
        for c in range(1, n_col):
            logs = logs + arrived_ref[c, :, width:]
        logdiag = logs[0:1, :nrhs] / width
        ones = jnp.ones((1, width), jnp.float32)
        squares = lax.dot_general(
            ones, solved * solved, TO_ROWS, precision=lax.Precision.HIGHEST, preferred_element_type=jnp.float32
        )
        loglik_out[...] = -0.5 * (squares / width) + logdiag - 0.5 * math.log(2.0 * math.pi)

    return call(body, (arrived,), (((nrhs, width), jnp.float32), ((1, nrhs), jnp.float32)))


def local(right_side, inverse_t, u_factor, v_factor, ranks):
    n = lax.axis_size(ROW)
    n_col = lax.axis_size(COL)
    nrhs, width = right_side.shape[2:]
    piece = width // n_col
    rank_max = u_factor.shape[4]
    col = lax.axis_index(COL)
    source = right_side.reshape(nrhs, width)
    u_tile = u_factor.reshape(rank_max, width)
    v_tile = v_factor.reshape(rank_max, width)
    keep = jnp.arange(rank_max, dtype=jnp.int32)[:, None] < ranks.reshape(1, 1)
    u_tile = jnp.where(keep, u_tile, jnp.zeros_like(u_tile))

    def move(array, pairs):
        numbered = [(s[0] * n_col + s[1], d[0] * n_col + d[1]) for s, d in pairs]
        return lax.ppermute(array, BOTH, numbered)

    rows = inverse_t.reshape(piece, width).astype(jnp.float32)
    quarter = width // SIDE
    slabs = []
    for k in range(SIDE):
        pairs = [
            ((r, x * SIDE + k), (r, x * SIDE + solver(r)[1] % SIDE))
            for r in range(n)
            for x in range(SIDE)
            if solver(r)[1] % SIDE != k
        ]
        slabs.append(move(rows, pairs) + jnp.where(col % SIDE == k, rows, 0.0))
    block = jnp.concatenate(slabs, axis=0)
    square = lax.dynamic_slice_in_dim(rows, col * piece, piece, 1)
    log_sum = jnp.broadcast_to(jnp.sum(jnp.log(jnp.diagonal(square))), (nrhs, 128))
    both = jnp.concatenate([v_tile, u_tile], axis=0).astype(jnp.float32)
    block, both, log_sum = lax.optimization_barrier((block, both, log_sum))
    parts = []
    for k in range(SIDE):
        pairs = [
            ((r, k * SIDE + solver(r)[1] % SIDE), solver(r)) for r in range(n) if solver(r)[1] // SIDE != k
        ]
        parts.append(move(block[:, k * quarter :], pairs))
    place = jnp.stack([col // SIDE]).astype(jnp.int32)

    moved = [both]
    for d in range(2, BAND + 1):
        moved.append(move(both, [((i, i - d), solver(i)) for i in range(d, n)]))
    inverse = assemble(place, block, parts)

    chain, odd, even = plan(n)
    nothing = jnp.zeros((nrhs, width), jnp.float32)
    came = jnp.zeros((BAND, nrhs, width), jnp.float32)
    v_band, u_band = [], []
    pending, base = prepare(-1, nothing, nothing, nothing, source, inverse)
    send, own = step(-1, came, came, nothing, base, v_tile, u_tile, v_band, u_band)
    odds = evens = nothing
    for r in range(n - 1):
        came = move(send, chain[r])
        more_odds = more_evens = nothing
        if 3 <= r < n - 2:
            more_odds = move(own, odd[r])
        if 2 <= r < n - 2:
            more_evens = move(own, even[r])
        if r < BAND:
            v_held, u_held = settle(moved[r], inverse)
            v_band.append(v_held)
            u_band.append(u_held)
        pending, base = prepare(r, odds, evens, pending, source, inverse)
        send, own = step(r, came, send, own, base, v_tile, u_tile, v_band, u_band)
        odds, evens = more_odds, more_evens

    payload = spread_out(send, log_sum, n_col)
    arrived = lax.all_to_all(payload, COL, 0, 0, tiled=True)
    solved, loglik = finish(arrived, width)
    return solved.reshape(1, 1, nrhs, width), loglik.reshape(1, 1, nrhs)


def solution(mesh):
    plane = Mesh(mesh.devices.reshape(-1, SIDE, SIDE), BOTH)
    return jax.shard_map(
        local,
        mesh=plane,
        in_specs=(
            P(None, ROW, None, None),
            P(None, ROW, COL, None),
            P(None, ROW, None, COL, None, None),
            P(None, ROW, None, COL, None, None),
            P(None, ROW, None, COL),
        ),
        out_specs=(P(None, ROW, None, None), P(None, ROW, None)),
        check_vma=False,
    )
```

```python
import math

import jax
import jax.numpy as jnp
from jax import lax
from jax.experimental import pallas as pl
from jax.experimental.pallas import tpu as pltpu
from jax.sharding import Mesh
from jax.sharding import PartitionSpec as P


ROW = "row"
COL = ("col_x", "col_y")
BOTH = (ROW, *COL)
SIDE = 4
BAND = 3
FAR_PERIOD = 6
ARRIVAL = {4: 1, 5: 2, 6: 2, 7: 3, 8: 3, 9: 3, 10: 4, 11: 4, 12: 4, 13: 4, 14: 4, 15: 4}
SENDER = {4: 1, 5: 1, 6: 4, 7: 4, 8: 5, 9: 6, 10: 4, 11: 5, 12: 6, 13: 7, 14: 8, 15: 9}


def solver(i):
    return (i, i - 2 if i >= 2 else i)


def union(rounds, kinds):
    patterns = {}
    for kind in sorted(set(kinds)):
        pairs = sorted({pair for moves, its in zip(rounds, kinds) if its == kind for pair in moves})
        assert len({s for s, _ in pairs}) == len(pairs) == len({d for _, d in pairs})
        patterns[kind] = pairs
    return [patterns[kind] for kind in kinds]


def plan(n):
    chain, odd, even = [], [], []
    for r in range(n - 1):
        chain.append([(solver(r), solver(r + 1))])
        odd.append([])
        even.append([])
        for i in range(n):
            for j in range(i - BAND):
                d = i - j
                if j + ARRIVAL[d] == r:
                    chain[r].append((solver(j) if SENDER[d] == 1 else (j + SENDER[d], j), (i, j)))
                if i - 2 - (d - 4) // 2 == r:
                    (odd if d % 2 else even)[r].append(((i, j), solver(i)))
    last = [*range(n - 4), 0, n - 4, n - 4]
    far = [r % FAR_PERIOD for r in range(n - 1)]
    return union(chain, last), union(odd, far), union(even, far)


VMEM = pl.BlockSpec(memory_space=pltpu.VMEM)
TO_ROWS = (((1,), (1,)), ((), ()))


def call(body, inputs, shapes, limit=8):
    return pl.pallas_call(
        body,
        in_specs=[VMEM] * len(inputs),
        out_specs=[VMEM] * len(shapes),
        out_shape=[jax.ShapeDtypeStruct(shape, dtype) for shape, dtype in shapes],
        compiler_params=pltpu.CompilerParams(vmem_limit_bytes=limit * 2**20),
    )(*inputs)


def here():
    row = lax.axis_index(ROW)
    col = lax.axis_index(COL[0]) * SIDE + lax.axis_index(COL[1])
    return row, col


def in_turn(now):
    row, col = here()
    return (row == now + 1) & (col == solver(now + 1)[1])


def through(lhs, inverse_ref, block=256):
    width = inverse_ref.shape[1]
    columns = [
        jnp.dot(lhs[:, : n + block], inverse_ref[: n + block, n : n + block], preferred_element_type=jnp.float32)
        for n in range(0, width, block)
    ]
    return jnp.concatenate(columns, axis=1)


def regroup(rows, slabs):
    piece, width = rows.shape
    quarter = width // SIDE

    def body(rows_ref, *refs):
        mine = lax.axis_index(COL[1])
        for k in range(SIDE):
            slab = refs[k][...] + jnp.where(mine == k, rows_ref[...], 0.0)
            for x in range(SIDE):
                refs[SIDE + x][k * piece : (k + 1) * piece] = slab[:, x * quarter :]

    shapes = tuple(((quarter, width - x * quarter), jnp.float32) for x in range(SIDE))
    return call(body, (rows, *slabs), shapes)


def assemble(blocks, parts):
    quarter, width = blocks[0].shape

    def body(*refs):
        out = refs[-1]
        mine = lax.axis_index(COL[0])
        for k in range(SIDE):
            start = k * quarter
            got = jnp.where(mine == k, refs[k][...], 0.0)
            if k:
                got = got + refs[SIDE + k - 1][...]
                out[start : start + quarter, :start] = jnp.zeros((quarter, start), jnp.bfloat16)
            out[start : start + quarter, start:] = got.astype(jnp.bfloat16)

    return call(body, (*blocks, *parts), (((width, width), jnp.bfloat16),), 16)[0]


def complete(inverse, part):
    quarter = part.shape[0]

    def body(inverse_ref, part_ref, out):
        out[:quarter] = (inverse_ref[:quarter].astype(jnp.float32) + part_ref[...]).astype(jnp.bfloat16)
        out[quarter:] = inverse_ref[quarter:]

    return call(body, (inverse, part), ((inverse.shape, jnp.bfloat16),))[0]


def settle(factors, inverse):
    rank_max, width = factors.shape[0] // 2, factors.shape[1]

    def body(factors_ref, inverse_ref, v_out, u_out):
        v_out[...] = factors_ref[:rank_max].astype(jnp.bfloat16)
        u_out[...] = through(factors_ref[rank_max:].astype(jnp.bfloat16), inverse_ref).astype(jnp.bfloat16)

    shape = ((rank_max, width), jnp.bfloat16)
    return call(body, (factors, inverse), (shape, shape))


def prepare(now, odds, evens, pending, source, inverse):
    nrhs, width = source.shape

    def body(odds_ref, evens_ref, pending_ref, source_ref, inverse_ref, pending_out, base_out):
        row, col = here()
        behind = row - 1 - now
        adds = (row - col == 2) & (behind >= 0)
        left = pending_ref[...]
        if now >= 3:
            left = left + jnp.where(adds & (4 + 2 * behind <= row), evens_ref[...], 0.0)
        if now >= 4:
            left = left + jnp.where(adds & (5 + 2 * behind <= row), odds_ref[...], 0.0)
        pending_out[...] = left

        @pl.when(in_turn(now))
        def _():
            total = source_ref[...] - left
            high = total.astype(jnp.bfloat16)
            low = (total - high.astype(jnp.float32)).astype(jnp.bfloat16)
            base_out[...] = through(high, inverse_ref) + through(low, inverse_ref)

    small = ((nrhs, width), jnp.float32)
    return call(body, (odds, evens, pending, source, inverse), (small, small))


def step(now, came, send, own, base, v_tile, u_tile, v_band, u_band):
    held = max(0, min(BAND, now + 1))
    nrhs, width = base.shape

    def body(came_ref, send_ref, own_ref, base_ref, v_ref, u_ref, *refs):
        v_refs, u_refs = refs[:held], refs[held : 2 * held]
        send_out, own_out = refs[2 * held :]
        row, col = here()
        gap = row - col
        turn = in_turn(now)
        hears = row < 0
        for when in sorted(set(ARRIVAL.values())):
            gaps = [d for d in ARRIVAL if ARRIVAL[d] == when]
            hears = hears | ((gap >= min(gaps)) & (gap <= max(gaps)) & (col == now - when))

        def share(known, v, u):
            inner = lax.dot_general(known.astype(jnp.bfloat16), v[...], TO_ROWS, preferred_element_type=jnp.float32)
            return jnp.dot(inner.astype(jnp.bfloat16), u[...], preferred_element_type=jnp.float32)

        @pl.when(jnp.logical_not(turn))
        def _():
            for d in range(1, BAND):
                send_out[d] = jnp.zeros((nrhs, width), jnp.float32)

        @pl.when(jnp.logical_not(turn | hears))
        def _():
            send_out[0] = send_ref[0]
            own_out[...] = own_ref[...]

        @pl.when(hears)
        def _():
            send_out[0] = came_ref[0]
            own_out[...] = share(came_ref[0], v_ref, u_ref)

        @pl.when(turn)
        def _():
            total = base_ref[...]
            for d in range(held):
                total = total - share(came_ref[d], v_refs[d], u_refs[d])
            send_out[0] = total
            for d in range(1, BAND):
                send_out[d] = came_ref[d - 1]
            own_out[...] = own_ref[...]

    inputs = (came, send, own, base, v_tile, u_tile, *v_band[:held], *u_band[:held])
    return call(body, inputs, (((BAND, nrhs, width), jnp.float32), ((nrhs, width), jnp.float32)))


def spread_out(send, log_sum, n_col):
    nrhs, width = send.shape[1:]

    def body(send_ref, log_ref, out):
        for c in range(n_col):
            out[c, :, :width] = send_ref[0]
            out[c, :, width:] = log_ref[...]

    return call(body, (send, log_sum), (((n_col, nrhs, width + 128), jnp.float32),))[0]


def finish(arrived, width):
    n_col, nrhs = arrived.shape[:2]

    def body(arrived_ref, solved_out, loglik_out):
        row, _ = here()
        solved = arrived_ref[jnp.where(row < 2, row, row - 2), :, :width]
        solved_out[...] = solved
        logs = arrived_ref[0, :, width:]
        for c in range(1, n_col):
            logs = logs + arrived_ref[c, :, width:]
        logdiag = logs[0:1, :nrhs] / width
        ones = jnp.ones((1, width), jnp.float32)
        squares = lax.dot_general(
            ones, solved * solved, TO_ROWS, precision=lax.Precision.HIGHEST, preferred_element_type=jnp.float32
        )
        loglik_out[...] = -0.5 * (squares / width) + logdiag - 0.5 * math.log(2.0 * math.pi)

    return call(body, (arrived,), (((nrhs, width), jnp.float32), ((1, nrhs), jnp.float32)))


def local(right_side, inverse_t, u_factor, v_factor, ranks):
    n = lax.axis_size(ROW)
    n_col = lax.axis_size(COL)
    nrhs, width = right_side.shape[2:]
    piece = width // n_col
    rank_max = u_factor.shape[4]
    col = lax.axis_index(COL)
    source = right_side.reshape(nrhs, width)
    u_tile = u_factor.reshape(rank_max, width)
    v_tile = v_factor.reshape(rank_max, width)
    keep = jnp.arange(rank_max, dtype=jnp.int32)[:, None] < ranks.reshape(1, 1)
    u_tile = jnp.where(keep, u_tile, jnp.zeros_like(u_tile))

    def move(array, pairs):
        numbered = [(s[0] * n_col + s[1], d[0] * n_col + d[1]) for s, d in pairs]
        return lax.ppermute(array, BOTH, numbered)

    rows = inverse_t.reshape(piece, width).astype(jnp.float32)
    slabs = []
    for k in range(SIDE):
        pairs = [
            ((r, x * SIDE + k), (r, x * SIDE + solver(r)[1] % SIDE))
            for r in range(n)
            for x in range(SIDE)
            if solver(r)[1] % SIDE != k
        ]
        slabs.append(move(rows, pairs))
    square = lax.dynamic_slice_in_dim(rows, col * piece, piece, 1)
    log_sum = jnp.broadcast_to(jnp.sum(jnp.log(jnp.diagonal(square))), (nrhs, 128))
    both = jnp.concatenate([v_tile, u_tile], axis=0).astype(jnp.float32)
    slabs, both, log_sum = lax.optimization_barrier((slabs, both, log_sum))
    blocks = regroup(rows, slabs)
    parts = []
    for k in range(SIDE):
        pairs = [
            ((r, k * SIDE + solver(r)[1] % SIDE), solver(r)) for r in range(n) if solver(r)[1] // SIDE != k
        ]
        parts.append(move(blocks[k], pairs))

    moved = []
    for d in range(1, BAND + 1):
        if d == 2:
            moved.append(both)
            continue
        moved.append(move(both, [((i, i - d), solver(i)) for i in range(d, n)]))
    inverse = assemble(blocks, parts[1:])

    chain, odd, even = plan(n)
    nothing = jnp.zeros((nrhs, width), jnp.float32)
    came = jnp.zeros((BAND, nrhs, width), jnp.float32)
    v_band, u_band = [], []
    pending, base = prepare(-1, nothing, nothing, nothing, source, inverse)
    send, own = step(-1, came, came, nothing, base, v_tile, u_tile, v_band, u_band)
    odds = evens = nothing
    for r in range(n - 1):
        came = move(send, chain[r])
        more_odds = more_evens = nothing
        if 3 <= r < n - 2:
            more_odds = move(own, odd[r])
        if 2 <= r < n - 2:
            more_evens = move(own, even[r])
        if r < BAND:
            v_held, u_held = settle(moved[r], inverse)
            v_band.append(v_held)
            u_band.append(u_held)
        if r == BAND:
            inverse = complete(inverse, parts[0])
            for d in range(BAND):
                v_band[d], u_band[d] = settle(moved[d], inverse)
        pending, base = prepare(r, odds, evens, pending, source, inverse)
        send, own = step(r, came, send, own, base, v_tile, u_tile, v_band, u_band)
        odds, evens = more_odds, more_evens

    payload = spread_out(send, log_sum, n_col)
    arrived = lax.all_to_all(payload, COL, 0, 0, tiled=True)
    solved, loglik = finish(arrived, width)
    return solved.reshape(1, 1, nrhs, width), loglik.reshape(1, 1, nrhs)


def solution(mesh):
    plane = Mesh(mesh.devices.reshape(-1, SIDE, SIDE), BOTH)
    return jax.shard_map(
        local,
        mesh=plane,
        in_specs=(
            P(None, ROW, None, None),
            P(None, ROW, COL, None),
            P(None, ROW, None, COL, None, None),
            P(None, ROW, None, COL, None, None),
            P(None, ROW, None, COL),
        ),
        out_specs=(P(None, ROW, None, None), P(None, ROW, None)),
        check_vma=False,
    )
```
